32 devices in a mesh: tm: 8 (over z, y), sym: 4 (over x, core).
Axes of the slice: x: 2, y: 2, z: 4, core: 2. Of those that a mesh axis runs over, the one named last changes fastest.
Arguments:
- trade_age: float32 [65536], P(('tm', 'sym')), may hold values from 0.02 to 20
- trade_size: float32 [65536], P(('tm', 'sym')), may hold values from 0.5 to 4
- owner: int32 [65536, 1], P(('tm', 'sym')), may hold values from 0 to 31; in each aligned block of 2048 rows (0 to 2047, 2048 to 4095, ...) at most 96 rows name the same one
- symbol_lane: int32 [65536], P(('tm', 'sym')), may hold values from 0 to 15
- quote_offset: int32 [65536], P(('tm', 'sym')), may hold values from 0 to 511
- quotes: float32 [64, 4096, 128], P('sym', 'tm'), may hold values from -6 to 6
- rates: float32 [128], replicated, may hold values from 0.05 to 2
Outputs:
- joined: float32 [65536, 128], P(('tm', 'sym'))
The draws below stay inside these ranges and needn't reach their ends.
Inputs may be any that keep to these rules, and one draw needn't show every extreme that they name: Among the 2048 trades of one device no owner is named more than 96 times, and in every draw some device names some owner exactly 96 times. Owner o holds symbols of group o % 4 and quote rows of block o // 4.
All inputs are finite; a program needn't handle non-finite values.
Results may differ from the reference program's by a relative error of at most 0.00002.
Values sent between devices are 32-bit elements; how exact they have to be, the bound alone decides.
A program may use at most 64 MiB of HBM per device.

```python
import math
import jax
import jax.numpy as jnp
import numpy as np

F = 128
TICK_DEV = 2048
SYM_DEV = 16
QT_DEV = 512
TICKS = 65536
SYMS = 64
QT = 4096
CAP = 96
N_SYM = 4
DEVICES = 32


def set_ends(values, own_key, smallest, high):
    extent = values.shape
    index_at = [jax.random.randint(jax.random.fold_in(own_key, axis), (), 0, extent[axis]) for axis in range(len(extent))]
    values = values.at[tuple(index_at)].set(smallest)
    longest = extent.index(max(extent))
    index_at[longest] = (index_at[longest] + 1) % extent[longest]
    return values.at[tuple(index_at)].set(high)


def level_of(stream_key, extent, pieces, low, high):
    factor_of, own = 1.0, jax.random.fold_in(stream_key, 6)
    for dim, shards_of in pieces:
        heights = jnp.exp(jax.random.uniform(jax.random.fold_in(own, dim), (shards_of,), jnp.float32, low / len(pieces), high / len(pieces)))
        factor_of = factor_of * jnp.repeat(heights, extent[dim] // shards_of).reshape([-1 if axis == dim else 1 for axis in range(len(extent))])
    return factor_of


def deal_out(key, own, number, rows, number_of, top, bound, skew):
    sequence = jax.random.permutation(key, number_of)
    heavy_load, ordinary = load_shares(number_of, rows * top, bound, skew, True), load_shares(number_of, rows * top, bound, skew, False)
    places = jnp.arange(number_of)

    def named(sizes, offset_by):
        used = int((sizes > 0).sum())
        fixed = max(1, used // 4)
        shifted = fixed + (places - fixed + offset_by * (used - fixed)) % max(1, number_of - fixed)
        return jnp.zeros((number_of,), jnp.int32).at[sequence[jnp.where(places < fixed, places, shifted)]].set(jnp.asarray(sizes, jnp.int32))

    sizes = jnp.where(number % 4 == 0, named(heavy_load, number // 4), named(ordinary, number - number // 4 - 1))
    mixed = jax.random.permutation(jax.random.fold_in(own, 3), number_of)
    giver, sink = mixed[0:number_of // 2 * 2:2], mixed[1:number_of // 2 * 2:2]
    margin = jnp.minimum(sizes[giver] - 1, bound - sizes[sink]) // 2
    margin = jnp.where((giver == sequence[0]) | (sink == sequence[0]) | (sizes[sink] == 0), 0, jnp.maximum(margin, 0))
    shifted = jax.random.randint(jax.random.fold_in(own, 4), (number_of // 2,), 0, 1 << 20) % (margin + 1)
    sizes = sizes.at[giver].add(-shifted).at[sink].add(shifted)
    labels = jnp.searchsorted(jnp.cumsum(sizes), jnp.arange(rows * top), side="right").astype(jnp.int32)
    listing = labels.reshape(top, rows).T
    listing = listing[jax.random.permutation(jax.random.fold_in(own, 1), rows)]
    offset_by = jax.random.randint(jax.random.fold_in(own, 2), (rows, 1), 0, top)
    return jnp.take_along_axis(listing, (jnp.arange(top)[None, :] + offset_by) % top, axis=1)


def load_shares(amount, total, most, lean, full):
    portions = [(1 << 20) // math.isqrt(rank ** lean) + 1 for rank in range(1, amount + 1)]
    largest = most if full else min(most, max(-(-total // amount), total * portions[0] // sum(portions)))
    least = 1 if total - largest >= amount - 1 else 0
    counts, surplus = [largest] + [least] * (amount - 1), total - largest - least * (amount - 1)
    while surplus > 0:
        free = [i for i in range(1, amount) if counts[i] < largest] or [i for i in range(1, amount) if counts[i] < most]
        mass, budget = sum([portions[i] for i in free]), surplus
        for i in free:
            more = min(most - counts[i], max(1, budget * portions[i] // mass), surplus)
            counts[i] = counts[i] + more
            surplus = surplus - more
    return np.array(counts)


def gaussian(rng, extent, width, most, cuts=(), kind=jnp.bfloat16):
    array = width * jax.random.normal(rng, extent, jnp.float32)
    if cuts:
        array = array * level_of(rng, extent, cuts, -0.22, 0.18)
    return jnp.clip(array, -most, most).astype(kind)


def setup_inputs(seed: int = 0) -> dict:
    arg_keys = jax.random.split(jax.random.key(seed), 8)
    trade_age = jnp.clip(jnp.exp(math.log(20.0) - 6.9077553 * jax.random.uniform(arg_keys[0], (TICKS,), jnp.float32) ** level_of(arg_keys[0], (TICKS,), ((0, 32),), -0.2, 0.2)), 0.02, 20.0)
    trade_size = jnp.clip(jnp.exp(math.log(4.0) - 2.0794415 * jax.random.uniform(arg_keys[1], (TICKS,), jnp.float32) ** level_of(arg_keys[1], (TICKS,), ((0, 32),), -0.2, 0.2)), 0.5, 4.0)
    owner_keys = jax.random.split(jax.random.fold_in(arg_keys[2], 1), TICKS // TICK_DEV)
    owner_turns = jax.random.permutation(jax.random.fold_in(arg_keys[2], 3), TICKS // TICK_DEV)
    owner = jax.vmap(lambda own, number: deal_out(jax.random.fold_in(arg_keys[2], 2), own, number, TICK_DEV, DEVICES, 1, CAP, 2))(owner_keys, owner_turns).reshape((TICKS, 1))
    symbol_lane = set_ends(jax.random.randint(arg_keys[3], (TICKS,), 0, SYM_DEV), jax.random.fold_in(arg_keys[3], 1), 0, SYM_DEV - 1).astype(jnp.int32)
    quote_offset = set_ends(jax.random.randint(arg_keys[4], (TICKS,), 0, QT_DEV), jax.random.fold_in(arg_keys[4], 1), 0, QT_DEV - 1).astype(jnp.int32)
    quotes = gaussian(arg_keys[5], (SYMS, QT, F), 1.0, 6.0, ((0, 4), (1, 8)), jnp.float32)
    rates = jnp.clip(jnp.exp(jax.random.uniform(arg_keys[6], (F,), jnp.float32, math.log(0.05), math.log(2.0))), 0.05, 2.0)
    return {"trade_age": trade_age, "trade_size": trade_size, "owner": owner, "symbol_lane": symbol_lane, "quote_offset": quote_offset, "quotes": quotes, "rates": rates}


def reference(trade_age, trade_size, owner, symbol_lane, quote_offset, quotes, rates):
    target = owner[:, 0]
    symbol = ((target % N_SYM) * SYM_DEV + symbol_lane).astype(jnp.int32)
    quote_row = ((target // N_SYM) * QT_DEV + quote_offset).astype(jnp.int32)
    current = quotes[symbol, quote_row]
    earlier = jnp.maximum(quote_row - 1, 0).astype(jnp.int32)
    previous = jnp.where((quote_row > 0)[:, None], quotes[symbol, earlier], jnp.zeros_like(current))
    weight = jnp.exp(-trade_age[:, None] * rates[None, :])
    return trade_size[:, None] * (weight * current + (1.0 - weight) * previous)
```

```python
import functools

import jax
import jax.numpy as jnp
from jax import lax
from jax.experimental import pallas as pl
from jax.experimental.pallas import tpu as pltpu
from jax.sharding import PartitionSpec as P

LANES = 128
PAD = 8
MESH = pl.DeviceIdType.MESH


def partner(me, k, devices):
    if devices & (devices - 1):
        return (me + k) % devices
    out, bit = 0, 1
    while bit < devices:
        out = out + ((me // bit) % 2 + (k // bit) % 2) % 2 * bit
        bit *= 2
    return out


def join_kernel(
    cfg,
    owner_ref, lane_ref, offset_ref, age_ref, rates_ref, quotes_ref,
    out_ref,
    table, recv, sbuf, msg, got, rows_v, rows_s, slot_v, slot_s, cur, prev, bsend, brecv,
    qsem, bsem, msend, mrecv, jsend, jrecv, ssem,
):
    tm_n, sym_n, cap = cfg
    devices = tm_n * sym_n
    ticks = owner_ref.shape[1]
    lane_count, quote_rows, features = quotes_ref.shape
    stride = quote_rows + PAD
    tm, sym = lax.axis_index("tm"), lax.axis_index("sym")
    me = tm * sym_n + sym

    def device(p):
        return (p // sym_n, p % sym_n)

    loads = [
        pltpu.make_async_copy(
            quotes_ref.at[lane], table.at[pl.ds(lane * stride + PAD, quote_rows)], qsem.at[lane]
        )
        for lane in range(lane_count)
    ]
    for load in loads:
        load.start()

    barrier = pltpu.get_barrier_semaphore()

    @pl.loop(1, devices)
    def _(k):
        pl.semaphore_signal(
            barrier, inc=1, device_id=device(partner(me, k, devices)), device_id_type=MESH
        )

    owner = owner_ref[...]
    mine = owner == lax.broadcasted_iota(jnp.int32, (devices, ticks), 0)
    hot = mine.astype(jnp.float32)
    hot_b = hot.astype(jnp.bfloat16)
    width = 256 if ticks % 256 == 0 else 128
    upper = (
        lax.broadcasted_iota(jnp.int32, (width, width), 0)
        < lax.broadcasted_iota(jnp.int32, (width, width), 1)
    ).astype(jnp.float32).astype(jnp.bfloat16)
    base = jnp.zeros((devices, 1), jnp.float32)
    ranks = []
    for start in range(0, ticks, width):
        part = hot[:, start:start + width]
        before = jnp.dot(
            hot_b[:, start:start + width], upper, preferred_element_type=jnp.float32
        )
        ranks.append(jnp.sum(part * (before + base), axis=0, keepdims=True))
        base = base + jnp.sum(part, axis=1, keepdims=True)
    rank = jnp.concatenate(ranks, axis=1)
    slot_v[...] = jnp.clip(owner * cap + rank.astype(jnp.int32), 0, devices * cap - 1)
    slot_copy = pltpu.make_async_copy(slot_v, slot_s, ssem.at[0])
    slot_copy.start()

    place = (
        rank.astype(jnp.int32) == lax.broadcasted_iota(jnp.int32, (LANES, ticks), 0)
    ).astype(jnp.float32).astype(jnp.bfloat16)
    local = lane_ref[...] * stride + PAD - 1 + offset_ref[...]
    age = age_ref[...]
    high = age.astype(jnp.bfloat16).astype(jnp.float32)
    middle = (age - high).astype(jnp.bfloat16).astype(jnp.float32)
    low = age - high - middle
    pieces = [
        (local // LANES).astype(jnp.float32), (local % LANES).astype(jnp.float32), high, middle, low
    ]
    spread = jnp.concatenate([(hot * piece).astype(jnp.bfloat16) for piece in pieces], axis=0)
    put = lax.dot_general(
        spread, place, (((1,), (1,)), ((), ())), preferred_element_type=jnp.float32
    )
    taken = [put[i * devices:(i + 1) * devices] for i in range(5)]
    msg[:, 0, 0:LANES] = taken[0] * LANES + taken[1]
    msg[:, 0, LANES:2 * LANES] = (taken[2] + taken[3]) + taken[4]

    for load in loads:
        load.wait()
    for lane in range(lane_count):
        bsend[lane:lane + 1, :] = table[(lane + 1) * stride - 1:(lane + 1) * stride, :]
    pl.semaphore_wait(barrier, devices - 1)

    def boundary():
        return pltpu.make_async_remote_copy(
            src_ref=bsend, dst_ref=brecv, send_sem=bsem.at[0], recv_sem=bsem.at[1],
            device_id=(lax.rem(tm + 1, tm_n), sym), device_id_type=MESH,
        )

    @pl.when(tm < tm_n - 1)
    def _():
        boundary().start()

    def message(p):
        return pltpu.make_async_remote_copy(
            src_ref=msg.at[p], dst_ref=got.at[me], send_sem=msend.at[p], recv_sem=mrecv.at[me],
            device_id=device(p), device_id_type=MESH,
        )

    def message_in(p):
        return pltpu.make_async_remote_copy(
            src_ref=msg.at[p], dst_ref=got.at[p], send_sem=msend.at[p], recv_sem=mrecv.at[p],
            device_id=device(p), device_id_type=MESH,
        )

    @pl.loop(1, devices)
    def _(k):
        message(partner(me, devices - k, devices)).start()

    got[me] = msg[me]

    @pl.loop(1, devices)
    def _(k):
        message_in(partner(me, devices - k, devices)).wait_recv()

    rows_v[...] = jnp.clip(got[:, :, 0:LANES].astype(jnp.int32), 0, lane_count * stride - 2)
    rows_copy = pltpu.make_async_copy(rows_v, rows_s, ssem.at[1])
    rows_copy.start()

    @pl.when(tm > 0)
    def _():
        boundary().wait_recv()

    @pl.when(tm == 0)
    def _():
        brecv[...] = jnp.zeros_like(brecv)

    edge = brecv[...]
    for lane in range(lane_count):
        table[lane * stride + PAD - 1:lane * stride + PAD, :] = edge[lane:lane + 1, :]
    rows_copy.wait()

    rates = rates_ref[...]

    def joined(p):
        for r in range(cap):
            row = rows_s[p, 0, r]
            cur[r:r + 1, :] = table[pl.ds(row + 1, 1), :]
            prev[r:r + 1, :] = table[pl.ds(row, 1), :]
        ages = got[p, :, LANES:2 * LANES]
        ages = jnp.transpose(jnp.broadcast_to(ages, (LANES, LANES)))[:cap]
        weight = jnp.exp(-ages * rates)
        return weight * cur[...] + (1.0 - weight) * prev[...]

    def share(p, source):
        return pltpu.make_async_remote_copy(
            src_ref=sbuf.at[p],
            dst_ref=recv.at[pl.ds(pl.multiple_of(source * cap, 8), cap)],
            send_sem=jsend.at[p], recv_sem=jrecv.at[source],
            device_id=device(p), device_id_type=MESH,
        )

    @pl.loop(1, devices)
    def _(k):
        p = partner(me, devices - k, devices)
        sbuf[p] = joined(p)
        share(p, me).start()

    recv[pl.ds(pl.multiple_of(me * cap, 8), cap), :] = joined(me)
    slot_copy.wait()

    @pl.when(tm < tm_n - 1)
    def _():
        boundary().wait_send()

    @pl.loop(1, devices)
    def _(k):
        p = partner(me, devices - k, devices)
        message(p).wait_send()
        share(p, p).wait_recv()

    unroll = 32

    @pl.loop(0, ticks // unroll)
    def _(b):
        start = pl.multiple_of(b * unroll, unroll)
        for u in range(unroll):
            out_ref[pl.ds(start + u, 1), :] = recv[pl.ds(slot_s[0, start + u], 1), :]

    @pl.loop(1, devices)
    def _(k):
        share(partner(me, devices - k, devices), me).wait_send()


def per_device(trade_age, trade_size, owner, symbol_lane, quote_offset, quotes, rates):
    tm_n, sym_n = lax.axis_size("tm"), lax.axis_size("sym")
    devices = tm_n * sym_n
    ticks = trade_age.shape[0]
    cap = 3 * ticks // (2 * devices)
    lane_count, quote_rows, features = quotes.shape
    vmem = pl.BlockSpec(memory_space=pltpu.VMEM)
    dma = pltpu.SemaphoreType.DMA
    joined = pl.pallas_call(
        functools.partial(join_kernel, (tm_n, sym_n, cap)),
        out_shape=jax.ShapeDtypeStruct((ticks, features), jnp.float32),
        in_specs=[vmem] * 5 + [pl.BlockSpec(memory_space=pl.ANY)],
        out_specs=vmem,
        scratch_shapes=[
            pltpu.VMEM((lane_count * (quote_rows + PAD), features), jnp.float32),
            pltpu.VMEM((devices * cap, features), jnp.float32),
            pltpu.VMEM((devices, cap, features), jnp.float32),
            pltpu.VMEM((devices, 1, 2 * LANES), jnp.float32),
            pltpu.VMEM((devices, 1, 2 * LANES), jnp.float32),
            pltpu.VMEM((devices, 1, LANES), jnp.int32),
            pltpu.SMEM((devices, 1, LANES), jnp.int32),
            pltpu.VMEM((1, ticks), jnp.int32),
            pltpu.SMEM((1, ticks), jnp.int32),
            pltpu.VMEM((cap, features), jnp.float32),
            pltpu.VMEM((cap, features), jnp.float32),
            pltpu.VMEM((lane_count, features), jnp.float32),
            pltpu.VMEM((lane_count, features), jnp.float32),
            dma((lane_count,)), dma((2,)),
            dma((devices,)), dma((devices,)), dma((devices,)), dma((devices,)),
            dma((2,)),
        ],
        compiler_params=pltpu.CompilerParams(collective_id=0, has_side_effects=True),
    )(
        owner.reshape(1, ticks), symbol_lane.reshape(1, ticks), quote_offset.reshape(1, ticks),
        trade_age.reshape(1, ticks), rates.reshape(1, features), quotes,
    )
    return trade_size[:, None] * joined


def solution(mesh):
    in_specs = (
        P(("tm", "sym")),
        P(("tm", "sym")),
        P(("tm", "sym"), None),
        P(("tm", "sym")),
        P(("tm", "sym")),
        P("sym", "tm", None),
        P(),
    )
    out_specs = P(("tm", "sym"), None)
    return jax.shard_map(
        per_device, mesh=mesh, in_specs=in_specs, out_specs=out_specs, check_vma=False
    )
```

```python
import functools

import jax
import jax.numpy as jnp
from jax import lax
from jax.experimental import pallas as pl
from jax.experimental.pallas import tpu as pltpu
from jax.sharding import PartitionSpec as P

LANES = 128
PAD = 8
MESH = pl.DeviceIdType.MESH


def flips(me, devices):
    out, bit = [], 1
    while bit < devices:
        out.append(bit - 2 * bit * lax.rem(lax.div(me, bit), 2))
        bit *= 2
    return out


def join_kernel(
    cfg,
    owner_ref, lane_ref, offset_ref, age_ref, rates_ref, quotes_ref,
    out_ref,
    table, recv, sbuf, msg, got, rows_v, rows_s, slot_v, slot_s, cur, prev, bsend, brecv,
    qsem, bsem, msend, mrecv, jsend, jrecv, ssem,
):
    tm_n, sym_n, cap = cfg
    devices = tm_n * sym_n
    ticks = owner_ref.shape[1]
    lane_count, quote_rows, features = quotes_ref.shape
    stride = quote_rows + PAD
    tm, sym = lax.axis_index("tm"), lax.axis_index("sym")
    me = tm * sym_n + sym

    flip = flips(me, devices)
    group = min(8, devices)

    def peer(k):
        p = me
        for i, step in enumerate(flip):
            if k >> i & 1:
                p = p + step
        return p

    def device(p):
        return (lax.div(p, sym_n), lax.rem(p, sym_n))

    everyone = range(devices - 1, 0, -1)

    loads = [
        pltpu.make_async_copy(
            quotes_ref.at[lane], table.at[pl.ds(lane * stride + PAD, quote_rows)], qsem.at[lane]
        )
        for lane in range(lane_count)
    ]
    for load in loads:
        load.start()

    barrier = pltpu.get_barrier_semaphore()

    for k in everyone:
        pl.semaphore_signal(barrier, inc=1, device_id=device(peer(k)), device_id_type=MESH)

    owner = owner_ref[...]
    mine = owner == lax.broadcasted_iota(jnp.int32, (devices, ticks), 0)
    hot = mine.astype(jnp.float32)
    hot_b = hot.astype(jnp.bfloat16)
    width = 256 if ticks % 256 == 0 else 128
    upper = (
        lax.broadcasted_iota(jnp.int32, (width, width), 0)
        < lax.broadcasted_iota(jnp.int32, (width, width), 1)
    ).astype(jnp.float32).astype(jnp.bfloat16)
    base = jnp.zeros((devices, 1), jnp.float32)
    ranks = []
    for start in range(0, ticks, width):
        part = hot[:, start:start + width]
        before = jnp.dot(
            hot_b[:, start:start + width], upper, preferred_element_type=jnp.float32
        )
        ranks.append(jnp.sum(part * (before + base), axis=0, keepdims=True))
        base = base + jnp.sum(part, axis=1, keepdims=True)
    rank = jnp.concatenate(ranks, axis=1)
    slot_v[...] = jnp.clip(owner * cap + rank.astype(jnp.int32), 0, devices * cap - 1)
    slot_copy = pltpu.make_async_copy(slot_v, slot_s, ssem.at[0])
    slot_copy.start()

    place = (
        rank.astype(jnp.int32) == lax.broadcasted_iota(jnp.int32, (LANES, ticks), 0)
    ).astype(jnp.float32).astype(jnp.bfloat16)
    local = lane_ref[...] * stride + PAD - 1 + offset_ref[...]
    age = age_ref[...]
    high = age.astype(jnp.bfloat16).astype(jnp.float32)
    middle = (age - high).astype(jnp.bfloat16).astype(jnp.float32)
    low = age - high - middle
    pieces = [
        (local // LANES).astype(jnp.float32), (local % LANES).astype(jnp.float32), high, middle, low
    ]
    spread = jnp.concatenate([(hot * piece).astype(jnp.bfloat16) for piece in pieces], axis=0)
    put = lax.dot_general(
        spread, place, (((1,), (1,)), ((), ())), preferred_element_type=jnp.float32
    )
    taken = [put[i * devices:(i + 1) * devices] for i in range(5)]
    msg[:, 0, 0:LANES] = taken[0] * LANES + taken[1]
    msg[:, 0, LANES:2 * LANES] = (taken[2] + taken[3]) + taken[4]

    def message(p):
        return pltpu.make_async_remote_copy(
            src_ref=msg.at[p], dst_ref=got.at[me], send_sem=msend.at[p], recv_sem=mrecv.at[me],
            device_id=device(p), device_id_type=MESH,
        )

    def message_in(p):
        return pltpu.make_async_remote_copy(
            src_ref=msg.at[p], dst_ref=got.at[p], send_sem=msend.at[p], recv_sem=mrecv.at[p],
            device_id=device(p), device_id_type=MESH,
        )

    pl.semaphore_wait(barrier, devices - 1)
    for k in everyone:
        message(peer(k)).start()
    got[me] = msg[me]

    for load in loads:
        load.wait()
    for lane in range(lane_count):
        bsend[lane:lane + 1, :] = table[(lane + 1) * stride - 1:(lane + 1) * stride, :]

    def boundary():
        return pltpu.make_async_remote_copy(
            src_ref=bsend, dst_ref=brecv, send_sem=bsem.at[0], recv_sem=bsem.at[1],
            device_id=(lax.rem(tm + 1, tm_n), sym), device_id_type=MESH,
        )

    @pl.when(tm < tm_n - 1)
    def _():
        boundary().start()

    @pl.when(tm == 0)
    def _():
        brecv[...] = jnp.zeros_like(brecv)

    @pl.when(tm > 0)
    def _():
        boundary().wait_recv()

    edge = brecv[...]
    for lane in range(lane_count):
        table[lane * stride + PAD - 1:lane * stride + PAD, :] = edge[lane:lane + 1, :]

    rates = rates_ref[...]

    def joined(p):
        for r in range(cap):
            row = rows_s[p, 0, r]
            cur[r:r + 1, :] = table[pl.ds(row + 1, 1), :]
            prev[r:r + 1, :] = table[pl.ds(row, 1), :]
        ages = got[p, :, LANES:2 * LANES]
        ages = jnp.transpose(jnp.broadcast_to(ages, (LANES, LANES)))[:cap]
        weight = jnp.exp(-ages * rates)
        return weight * cur[...] + (1.0 - weight) * prev[...]

    def share(p, source):
        return pltpu.make_async_remote_copy(
            src_ref=sbuf.at[p],
            dst_ref=recv.at[pl.ds(pl.multiple_of(source * cap, 8), cap)],
            send_sem=jsend.at[p], recv_sem=jrecv.at[source],
            device_id=device(p), device_id_type=MESH,
        )

    for g in range(devices // group - 1, -1, -1):
        lead = peer(g * group)
        for j in range(group - 1, -1, -1):
            if g or j:
                message_in(peer(g * group + j)).wait_recv()
        whole = pl.ds(pl.multiple_of(lax.div(lead, group) * group, group), group)
        rows_v[whole] = jnp.clip(
            got[whole, :, 0:LANES].astype(jnp.int32), 0, lane_count * stride - 2
        )
        rows_copy = pltpu.make_async_copy(rows_v.at[whole], rows_s.at[whole], ssem.at[1])
        rows_copy.start()
        rows_copy.wait()

        @pl.loop(0 if g else 1, group)
        def _(j, lead=lead):
            p, bit = lead, 1
            for step in flip[:group.bit_length() - 1]:
                p = p + lax.rem(lax.div(j, bit), 2) * step
                bit *= 2
            sbuf[p] = joined(p)
            share(p, me).start()

    recv[pl.ds(pl.multiple_of(me * cap, 8), cap), :] = joined(me)
    slot_copy.wait()

    @pl.when(tm < tm_n - 1)
    def _():
        boundary().wait_send()

    for k in everyone:
        message(peer(k)).wait_send()
    for k in everyone:
        share(peer(k), peer(k)).wait_recv()

    unroll = 32

    @pl.loop(0, ticks // unroll)
    def _(b):
        start = pl.multiple_of(b * unroll, unroll)
        for u in range(unroll):
            out_ref[pl.ds(start + u, 1), :] = recv[pl.ds(slot_s[0, start + u], 1), :]

    for k in everyone:
        share(peer(k), me).wait_send()


def per_device(trade_age, trade_size, owner, symbol_lane, quote_offset, quotes, rates):
    tm_n, sym_n = lax.axis_size("tm"), lax.axis_size("sym")
    devices = tm_n * sym_n
    ticks = trade_age.shape[0]
    cap = 3 * ticks // (2 * devices)
    lane_count, quote_rows, features = quotes.shape
    vmem = pl.BlockSpec(memory_space=pltpu.VMEM)
    dma = pltpu.SemaphoreType.DMA
    joined = pl.pallas_call(
        functools.partial(join_kernel, (tm_n, sym_n, cap)),
        out_shape=jax.ShapeDtypeStruct((ticks, features), jnp.float32),
        in_specs=[vmem] * 5 + [pl.BlockSpec(memory_space=pltpu.HBM)],
        out_specs=vmem,
        scratch_shapes=[
            pltpu.VMEM((lane_count * (quote_rows + PAD), features), jnp.float32),
            pltpu.VMEM((devices * cap, features), jnp.float32),
            pltpu.VMEM((devices, cap, features), jnp.float32),
            pltpu.VMEM((devices, 1, 2 * LANES), jnp.float32),
            pltpu.VMEM((devices, 1, 2 * LANES), jnp.float32),
            pltpu.VMEM((devices, 1, LANES), jnp.int32),
            pltpu.SMEM((devices, 1, LANES), jnp.int32),
            pltpu.VMEM((1, ticks), jnp.int32),
            pltpu.SMEM((1, ticks), jnp.int32),
            pltpu.VMEM((cap, features), jnp.float32),
            pltpu.VMEM((cap, features), jnp.float32),
            pltpu.VMEM((lane_count, features), jnp.float32),
            pltpu.VMEM((lane_count, features), jnp.float32),
            dma((lane_count,)), dma((2,)),
            dma((devices,)), dma((devices,)), dma((devices,)), dma((devices,)),
            dma((2,)),
        ],
        compiler_params=pltpu.CompilerParams(
            collective_id=0, has_side_effects=True, vmem_limit_bytes=60 << 20
        ),
    )(
        owner.reshape(1, ticks), symbol_lane.reshape(1, ticks), quote_offset.reshape(1, ticks),
        trade_age.reshape(1, ticks), rates.reshape(1, features), quotes,
    )
    return trade_size[:, None] * joined


def solution(mesh):
    in_specs = (
        P(("tm", "sym")),
        P(("tm", "sym")),
        P(("tm", "sym"), None),
        P(("tm", "sym")),
        P(("tm", "sym")),
        P("sym", "tm", None),
        P(),
    )
    out_specs = P(("tm", "sym"), None)
    return jax.shard_map(
        per_device, mesh=mesh, in_specs=in_specs, out_specs=out_specs, check_vma=False
    )
```

```python
import functools

import jax
import jax.numpy as jnp
from jax import lax
from jax.experimental import pallas as pl
from jax.experimental.pallas import tpu as pltpu
from jax.sharding import PartitionSpec as P

LANES = 128
PAD = 8
MESH = pl.DeviceIdType.MESH


def flips(me, devices):
    out, bit = [], 1
    while bit < devices:
        out.append(bit - 2 * bit * lax.rem(lax.div(me, bit), 2))
        bit *= 2
    return out


def join_kernel(
    cfg,
    owner_ref, lane_ref, offset_ref, age_ref, rates_ref, quotes_ref,
    out_ref,
    table, recv, sbuf, msg, got, rows_v, rows_s, slot_v, slot_s, cur, prev, bsend, brecv,
    qsem, bsem, msend, mrecv, jsend, jrecv, ssem,
):
    tm_n, sym_n, cap = cfg
    devices = tm_n * sym_n
    ticks = owner_ref.shape[1]
    lane_count, quote_rows, features = quotes_ref.shape
    stride = quote_rows + PAD
    tm, sym = lax.axis_index("tm"), lax.axis_index("sym")
    me = tm * sym_n + sym

    flip = flips(me, devices)
    group = min(8, devices)

    top = len(flip) - 1
    half = lax.div(2 * me, devices)
    quarter = lax.rem(lax.div(4 * me, devices), 2)

    def peer(k):
        p = me
        for i, step in enumerate(flip):
            if i == top - 1 and k >> top & 1:
                want = 1 - half if k >> i & 1 else half
                p = p + (want - quarter) * (1 << i)
            elif k >> i & 1:
                p = p + step
        return p

    def device(p):
        return (lax.div(p, sym_n), lax.rem(p, sym_n))

    everyone = range(devices - 1, 0, -1)

    loads = [
        pltpu.make_async_copy(
            quotes_ref.at[lane], table.at[pl.ds(lane * stride + PAD, quote_rows)], qsem.at[lane]
        )
        for lane in range(lane_count)
    ]
    for load in loads:
        load.start()

    barrier = pltpu.get_barrier_semaphore()

    for k in everyone:
        pl.semaphore_signal(barrier, inc=1, device_id=device(peer(k)), device_id_type=MESH)

    owner = owner_ref[...]
    mine = owner == lax.broadcasted_iota(jnp.int32, (devices, ticks), 0)
    hot = mine.astype(jnp.float32)
    hot_b = hot.astype(jnp.bfloat16)
    width = 256 if ticks % 256 == 0 else 128
    upper = (
        lax.broadcasted_iota(jnp.int32, (width, width), 0)
        < lax.broadcasted_iota(jnp.int32, (width, width), 1)
    ).astype(jnp.float32).astype(jnp.bfloat16)
    base = jnp.zeros((devices, 1), jnp.float32)
    ranks = []
    for start in range(0, ticks, width):
        part = hot[:, start:start + width]
        before = jnp.dot(
            hot_b[:, start:start + width], upper, preferred_element_type=jnp.float32
        )
        ranks.append(jnp.sum(part * (before + base), axis=0, keepdims=True))
        base = base + jnp.sum(part, axis=1, keepdims=True)
    rank = jnp.concatenate(ranks, axis=1)
    slot_v[...] = jnp.clip(owner * cap + rank.astype(jnp.int32), 0, devices * cap - 1)
    slot_copy = pltpu.make_async_copy(slot_v, slot_s, ssem.at[0])
    slot_copy.start()

    place = (
        rank.astype(jnp.int32) == lax.broadcasted_iota(jnp.int32, (LANES, ticks), 0)
    ).astype(jnp.float32).astype(jnp.bfloat16)
    local = lane_ref[...] * stride + PAD - 1 + offset_ref[...]
    age = age_ref[...]
    high = age.astype(jnp.bfloat16).astype(jnp.float32)
    middle = (age - high).astype(jnp.bfloat16).astype(jnp.float32)
    low = age - high - middle
    pieces = [
        (local // LANES).astype(jnp.float32), (local % LANES).astype(jnp.float32), high, middle, low
    ]
    spread = jnp.concatenate([(hot * piece).astype(jnp.bfloat16) for piece in pieces], axis=0)
    put = lax.dot_general(
        spread, place, (((1,), (1,)), ((), ())), preferred_element_type=jnp.float32
    )
    taken = [put[i * devices:(i + 1) * devices] for i in range(5)]
    msg[:, 0, 0:LANES] = taken[0] * LANES + taken[1]
    msg[:, 0, LANES:2 * LANES] = (taken[2] + taken[3]) + taken[4]

    def message(p):
        return pltpu.make_async_remote_copy(
            src_ref=msg.at[p], dst_ref=got.at[me], send_sem=msend.at[p], recv_sem=mrecv.at[me],
            device_id=device(p), device_id_type=MESH,
        )

    def message_in(p):
        return pltpu.make_async_remote_copy(
            src_ref=msg.at[p], dst_ref=got.at[p], send_sem=msend.at[p], recv_sem=mrecv.at[p],
            device_id=device(p), device_id_type=MESH,
        )

    pl.semaphore_wait(barrier, devices - 1)
    for k in everyone:
        message(peer(k)).start()
    got[me] = msg[me]

    for load in loads:
        load.wait()
    for lane in range(lane_count):
        bsend[lane:lane + 1, :] = table[(lane + 1) * stride - 1:(lane + 1) * stride, :]

    def boundary():
        return pltpu.make_async_remote_copy(
            src_ref=bsend, dst_ref=brecv, send_sem=bsem.at[0], recv_sem=bsem.at[1],
            device_id=(lax.rem(tm + 1, tm_n), sym), device_id_type=MESH,
        )

    @pl.when(tm < tm_n - 1)
    def _():
        boundary().start()

    @pl.when(tm == 0)
    def _():
        brecv[...] = jnp.zeros_like(brecv)

    @pl.when(tm > 0)
    def _():
        boundary().wait_recv()

    edge = brecv[...]
    for lane in range(lane_count):
        table[lane * stride + PAD - 1:lane * stride + PAD, :] = edge[lane:lane + 1, :]

    rates = rates_ref[...]

    def joined(p):
        for r in range(cap):
            row = rows_s[p, 0, r]
            cur[r:r + 1, :] = table[pl.ds(row + 1, 1), :]
            prev[r:r + 1, :] = table[pl.ds(row, 1), :]
        ages = got[p, :, LANES:2 * LANES]
        ages = jnp.transpose(jnp.broadcast_to(ages, (LANES, LANES)))[:cap]
        weight = jnp.exp(-ages * rates)
        return weight * cur[...] + (1.0 - weight) * prev[...]

    def share(p, source):
        return pltpu.make_async_remote_copy(
            src_ref=sbuf.at[p],
            dst_ref=recv.at[pl.ds(pl.multiple_of(source * cap, 8), cap)],
            send_sem=jsend.at[p], recv_sem=jrecv.at[source],
            device_id=device(p), device_id_type=MESH,
        )

    for g in range(devices // group - 1, -1, -1):
        lead = peer(g * group)
        for j in range(group - 1, -1, -1):
            if g or j:
                message_in(peer(g * group + j)).wait_recv()
        whole = pl.ds(pl.multiple_of(lax.div(lead, group) * group, group), group)
        rows_v[whole] = jnp.clip(
            got[whole, :, 0:LANES].astype(jnp.int32), 0, lane_count * stride - 2
        )
        rows_copy = pltpu.make_async_copy(rows_v.at[whole], rows_s.at[whole], ssem.at[1])
        rows_copy.start()
        rows_copy.wait()

        @pl.loop(0 if g else 1, group)
        def _(j, lead=lead):
            p, bit = lead, 1
            for step in flip[:group.bit_length() - 1]:
                p = p + lax.rem(lax.div(j, bit), 2) * step
                bit *= 2
            sbuf[p] = joined(p)
            share(p, me).start()

    recv[pl.ds(pl.multiple_of(me * cap, 8), cap), :] = joined(me)
    slot_copy.wait()

    @pl.when(tm < tm_n - 1)
    def _():
        boundary().wait_send()

    for k in everyone:
        message(peer(k)).wait_send()
    for k in everyone:
        share(peer(k), peer(k)).wait_recv()

    unroll = 32

    @pl.loop(0, ticks // unroll)
    def _(b):
        start = pl.multiple_of(b * unroll, unroll)
        for u in range(unroll):
            out_ref[pl.ds(start + u, 1), :] = recv[pl.ds(slot_s[0, start + u], 1), :]

    for k in everyone:
        share(peer(k), me).wait_send()


def per_device(trade_age, trade_size, owner, symbol_lane, quote_offset, quotes, rates):
    tm_n, sym_n = lax.axis_size("tm"), lax.axis_size("sym")
    devices = tm_n * sym_n
    ticks = trade_age.shape[0]
    cap = 3 * ticks // (2 * devices)
    lane_count, quote_rows, features = quotes.shape
    vmem = pl.BlockSpec(memory_space=pltpu.VMEM)
    dma = pltpu.SemaphoreType.DMA
    joined = pl.pallas_call(
        functools.partial(join_kernel, (tm_n, sym_n, cap)),
        out_shape=jax.ShapeDtypeStruct((ticks, features), jnp.float32),
        in_specs=[vmem] * 5 + [pl.BlockSpec(memory_space=pltpu.HBM)],
        out_specs=vmem,
        scratch_shapes=[
            pltpu.VMEM((lane_count * (quote_rows + PAD), features), jnp.float32),
            pltpu.VMEM((devices * cap, features), jnp.float32),
            pltpu.VMEM((devices, cap, features), jnp.float32),
            pltpu.VMEM((devices, 1, 2 * LANES), jnp.float32),
            pltpu.VMEM((devices, 1, 2 * LANES), jnp.float32),
            pltpu.VMEM((devices, 1, LANES), jnp.int32),
            pltpu.SMEM((devices, 1, LANES), jnp.int32),
            pltpu.VMEM((1, ticks), jnp.int32),
            pltpu.SMEM((1, ticks), jnp.int32),
            pltpu.VMEM((cap, features), jnp.float32),
            pltpu.VMEM((cap, features), jnp.float32),
            pltpu.VMEM((lane_count, features), jnp.float32),
            pltpu.VMEM((lane_count, features), jnp.float32),
            dma((lane_count,)), dma((2,)),
            dma((devices,)), dma((devices,)), dma((devices,)), dma((devices,)),
            dma((2,)),
        ],
        compiler_params=pltpu.CompilerParams(
            collective_id=0, has_side_effects=True, vmem_limit_bytes=60 << 20
        ),
    )(
        owner.reshape(1, ticks), symbol_lane.reshape(1, ticks), quote_offset.reshape(1, ticks),
        trade_age.reshape(1, ticks), rates.reshape(1, features), quotes,
    )
    return trade_size[:, None] * joined


def solution(mesh):
    in_specs = (
        P(("tm", "sym")),
        P(("tm", "sym")),
        P(("tm", "sym"), None),
        P(("tm", "sym")),
        P(("tm", "sym")),
        P("sym", "tm", None),
        P(),
    )
    out_specs = P(("tm", "sym"), None)
    return jax.shard_map(
        per_device, mesh=mesh, in_specs=in_specs, out_specs=out_specs, check_vma=False
    )
```
